32 devices in a mesh: rep: 1, dp: 32 (over x, y, z, core).
Axes of the slice: x: 2, y: 2, z: 4, core: 2. Of those that a mesh axis runs over, the one named last changes fastest.
Arguments:
- x: bfloat16 [32, 2048, 512], P(('rep', 'dp'))
- dy: bfloat16 [32, 2048, 512], P(('rep', 'dp'))
- wq: bfloat16 [2, 512, 512], replicated
- wk: bfloat16 [2, 512, 512], replicated
- wv: bfloat16 [2, 512, 512], replicated
- wo: bfloat16 [2, 512, 512], replicated
- w_gate: bfloat16 [2, 512, 2048], replicated
- w_up: bfloat16 [2, 512, 2048], replicated
- w_down: bfloat16 [2, 2048, 512], replicated
- m_wq: float32 [2, 512, 512], P(None, 'dp')
- m_wk: float32 [2, 512, 512], P(None, 'dp')
- m_wv: float32 [2, 512, 512], P(None, 'dp')
- m_wo: float32 [2, 512, 512], P(None, 'dp')
- m_w_gate: float32 [2, 512, 2048], P(None, 'dp')
- m_w_up: float32 [2, 512, 2048], P(None, 'dp')
- m_w_down: float32 [2, 2048, 512], P(None, 'dp')
- v_wq: float32 [2, 512, 512], P(None, 'dp')
- v_wk: float32 [2, 512, 512], P(None, 'dp')
- v_wv: float32 [2, 512, 512], P(None, 'dp')
- v_wo: float32 [2, 512, 512], P(None, 'dp')
- v_w_gate: float32 [2, 512, 2048], P(None, 'dp')
- v_w_up: float32 [2, 512, 2048], P(None, 'dp')
- v_w_down: float32 [2, 2048, 512], P(None, 'dp')
Outputs:
- output 1: bfloat16 [2, 512, 512], P('rep')
- output 2: bfloat16 [2, 512, 512], P('rep')
- output 3: bfloat16 [2, 512, 512], P('rep')
- output 4: bfloat16 [2, 512, 512], P('rep')
- output 5: bfloat16 [2, 512, 2048], P('rep')
- output 6: bfloat16 [2, 512, 2048], P('rep')
- output 7: bfloat16 [2, 2048, 512], P('rep')
- output 8: float32 [2, 512, 512], P('rep', 'dp')
- output 9: float32 [2, 512, 512], P('rep', 'dp')
- output 10: float32 [2, 512, 512], P('rep', 'dp')
- output 11: float32 [2, 512, 512], P('rep', 'dp')
- output 12: float32 [2, 512, 2048], P('rep', 'dp')
- output 13: float32 [2, 512, 2048], P('rep', 'dp')
- output 14: float32 [2, 2048, 512], P('rep', 'dp')
- output 15: float32 [2, 512, 512], P('rep', 'dp')
- output 16: float32 [2, 512, 512], P('rep', 'dp')
- output 17: float32 [2, 512, 512], P('rep', 'dp')
- output 18: float32 [2, 512, 512], P('rep', 'dp')
- output 19: float32 [2, 512, 2048], P('rep', 'dp')
- output 20: float32 [2, 512, 2048], P('rep', 'dp')
- output 21: float32 [2, 2048, 512], P('rep', 'dp')
All inputs are finite; a program needn't handle non-finite values.
Results may differ from the reference program's by a relative error of at most 0.0293.
Values are sent between devices in bfloat16 or wider.
A program may use at most 2 GiB of HBM per device.

```python
import jax
import jax.numpy as jnp
from jax import lax

SEQUENCES = 32
TOKENS = 2048
D = 512
HEADS = 2
KV_HEADS = 2
HEAD = 256
FF = 2048
LAYERS = 2
THETA = 10000
NAMES = ("wq", "wk", "wv", "wo", "w_gate", "w_up", "w_down")
SHAPES = {
    "wq": (LAYERS, D, HEADS * HEAD),
    "wk": (LAYERS, D, KV_HEADS * HEAD),
    "wv": (LAYERS, D, KV_HEADS * HEAD),
    "wo": (LAYERS, HEADS * HEAD, D),
    "w_gate": (LAYERS, D, FF),
    "w_up": (LAYERS, D, FF),
    "w_down": (LAYERS, FF, D),
}


def bump(key, n, height):
    away = (jnp.arange(n, dtype=jnp.int32) - jax.random.randint(key, (), 0, n, jnp.int32)) % n
    return jnp.where(away < n // 8, height, 1.0)


def together(key, own, strength):
    shared = jax.random.normal(key, own.shape[1:], jnp.float32)
    return (own + strength * shared) * lax.rsqrt(1 + strength * strength)


def setup_inputs(seed: int = 0, part: int = 0) -> dict:
    kx, kdy, ka, kb, kz, kf, kh, kl, *keys = jax.random.split(jax.random.key(seed), 8 + 3 * len(NAMES))
    kx, kdy, ka, kb = (jax.random.fold_in(k, part) for k in (kx, kdy, ka, kb))
    kw, km, kv = (keys[i::3] for i in range(3))
    shape = (SEQUENCES, TOKENS, D)
    much_x, much_dy = jax.random.uniform(kz, (2,), jnp.float32, 0.0, 1.0)
    loud = 2.0 ** jax.random.uniform(jax.random.fold_in(kz, 1), (), jnp.float32, -1.0, 2.0)
    layers = 2.0 ** jax.random.uniform(kl, (LAYERS, 1, 1), jnp.float32, -1.0, 1.0)
    times = {"wq": 1.0, "wk": 1.0, "wv": 2.0, "wo": layers, "w_gate": 1.0, "w_up": bump(kh, FF, 4.0), "w_down": layers}
    x = together(ka, jax.random.normal(kx, shape, jnp.float32), much_x) * bump(kf, D, 4.0)
    dy = together(kb, jax.random.normal(kdy, shape, jnp.float32), much_dy)
    drawn = {"x": x.astype(jnp.bfloat16), "dy": (loud * dy * (SEQUENCES * TOKENS) ** -0.5).astype(jnp.bfloat16)}
    for key, name in zip(kw, NAMES, strict=True):
        drawn[name] = (jax.random.normal(key, SHAPES[name], jnp.float32) * SHAPES[name][1] ** -0.5 * times[name]).astype(jnp.bfloat16)
    for key, name in zip(km, NAMES, strict=True):
        drawn[f"m_{name}"] = 0.1 * jax.random.normal(key, SHAPES[name], jnp.float32)
    for key, name in zip(kv, NAMES, strict=True):
        drawn[f"v_{name}"] = jax.random.uniform(key, SHAPES[name], jnp.float32, 0.02, 0.06)
    return drawn


def matmul(a, w):
    return jnp.dot(a, w, preferred_element_type=jnp.float32).astype(jnp.bfloat16)


def normed(h):
    wide = h.astype(jnp.float32)
    scale = lax.rsqrt(jnp.mean(wide**2, -1, keepdims=True) + 1e-6)
    return (wide * scale).astype(jnp.bfloat16)


def turned(t, theta):
    half = t.shape[-1] // 2
    angle = jnp.arange(t.shape[0], dtype=jnp.float32)[:, None] * theta ** (-jnp.arange(half, dtype=jnp.float32) / half)
    cos, sin = jnp.cos(angle)[:, None], jnp.sin(angle)[:, None]
    a, b = t[..., :half].astype(jnp.float32), t[..., half:].astype(jnp.float32)
    return jnp.concatenate([a * cos - b * sin, b * cos + a * sin], -1).astype(jnp.bfloat16)


def seen_by(q, k, v):
    tokens, kv = q.shape[0], k.shape[1]
    q = q.reshape(tokens, kv, -1, q.shape[-1])
    scores = jnp.einsum("tgsd,ugd->gstu", q.astype(jnp.float32), k.astype(jnp.float32)) * q.shape[-1] ** -0.5
    place = jnp.arange(tokens)
    weights = jax.nn.softmax(jnp.where(place[:, None] >= place, scores, -jnp.inf), -1).astype(jnp.bfloat16)
    return jnp.einsum("gstu,ugd->tgsd", weights.astype(jnp.float32), v.astype(jnp.float32)).astype(jnp.bfloat16).reshape(tokens, -1)


def layer(h, w):
    a = normed(h)
    q, k = (turned(matmul(a, w[name]).reshape(h.shape[0], -1, HEAD), THETA) for name in ("wq", "wk"))
    h = h + matmul(seen_by(q, k, matmul(a, w["wv"]).reshape(h.shape[0], -1, HEAD)), w["wo"])
    b = normed(h)
    gate = jnp.dot(b, w["w_gate"], preferred_element_type=jnp.float32)
    up = jnp.dot(b, w["w_up"], preferred_element_type=jnp.float32)
    return h + matmul((jax.nn.silu(gate) * up).astype(jnp.bfloat16), w["w_down"])


def adamw(w, m, v, g):
    m = 0.9 * m + 0.1 * g
    v = 0.95 * v + 0.05 * g * g
    step = m * lax.rsqrt(v + 1e-8) + 0.1 * w
    return (w - 0.02 * step).astype(jnp.bfloat16), m, v


def clipped(gradients, sum_of_squares, count):
    factor = jnp.minimum(1.0, 0.5 * lax.rsqrt(sum_of_squares / count + 1e-30))
    return [g * factor for g in gradients]


def stack(weights, h):
    return lax.scan(lambda h, w: (layer(h, w), None), h, weights)[0]


def reference(x, dy, wq, wk, wv, wo, w_gate, w_up, w_down, m_wq, m_wk, m_wv, m_wo, m_w_gate, m_w_up, m_w_down, v_wq, v_wk, v_wv, v_wo, v_w_gate, v_w_up, v_w_down):
    weights = dict(zip(NAMES, (wq, wk, wv, wo, w_gate, w_up, w_down), strict=True))

    def take(so_far, sequence):
        h, by_y = sequence
        _, back = jax.vjp(stack, weights, h)
        by_weights, by_h = back(by_y)
        return jax.tree.map(lambda total, term: total + term.astype(jnp.float32), so_far, by_weights), by_h

    none_yet = {name: jnp.zeros(w.shape, jnp.float32) for name, w in weights.items()}
    by_weights, by_x = lax.scan(take, none_yet, (x, dy))
    gradients = [by_weights[name].astype(jnp.bfloat16).astype(jnp.float32) for name in NAMES]
    gradients = clipped(gradients, sum(jnp.sum(g * g) for g in gradients), sum(g.size for g in gradients))
    first = (m_wq, m_wk, m_wv, m_wo, m_w_gate, m_w_up, m_w_down)
    second = (v_wq, v_wk, v_wv, v_wo, v_w_gate, v_w_up, v_w_down)
    new = [adamw(weights[name].astype(jnp.float32), m, v, g) for name, m, v, g in zip(NAMES, first, second, gradients, strict=True)]
    return tuple(one[which] for which in range(3) for one in new)
```

```python
import functools

import jax
import jax.numpy as jnp
from jax import lax
from jax.experimental import pallas as pl
from jax.experimental.pallas import tpu as pltpu
from jax.sharding import PartitionSpec as P

HEAD = 256
HALF = HEAD // 2
THETA = 10000
NAMES = ("wq", "wk", "wv", "wo", "w_gate", "w_up", "w_down")
NEG = -1e30
HIDDEN = 2 * NEG
LOG2E = 1.4426950408889634
VMEM = 56 * 2**20
BLOCK = 512
FWD_STRIPS = 4
SCALE = HEAD**-0.5


def _dot(a, b, ca, cb):
    return lax.dot_general(a, b, (((ca,), (cb,)), ((), ())), preferred_element_type=jnp.float32)


def _turn(t, cos, sin, back=False):
    a, b = t[:, :HALF].astype(jnp.float32), t[:, HALF:].astype(jnp.float32)
    if back:
        return jnp.concatenate([a * cos + b * sin, b * cos - a * sin], axis=1).astype(jnp.bfloat16)
    return jnp.concatenate([a * cos - b * sin, b * cos + a * sin], axis=1).astype(jnp.bfloat16)


def _head(i):
    return slice(i * HEAD, (i + 1) * HEAD)


def _turn_all(src, dst, cos_ref, sin_ref, heads, at, rows):
    def strip(s, _):
        here = pl.ds(pl.multiple_of(s * 256, 256), 256)
        place = pl.ds(pl.multiple_of(at + s * 256, 256), 256)
        for i in range(heads):
            dst[here, _head(i)] = _turn(src[here, _head(i)], cos_ref[place, :], sin_ref[place, :])
    lax.fori_loop(0, rows // 256, strip, None)


def _gap():
    return lax.broadcasted_iota(jnp.int32, (BLOCK, BLOCK), 1) - lax.broadcasted_iota(jnp.int32, (BLOCK, BLOCK), 0)


def _forward(q_ref, k_ref, v_ref, cos_ref, sin_ref, o_ref, lse_ref, qr_s, kr_s, top_s, mix_s, gap_s, *, heads):
    bq = q_ref.shape[0]
    strips = bq // BLOCK
    iq = pl.program_id(0)
    e = SCALE * LOG2E
    pieces = [(i, n) for n in range(strips) for i in range(heads)]

    @pl.when(iq == 0)
    def _():
        gap_s[...] = _gap()
        _turn_all(k_ref, kr_s, cos_ref, sin_ref, heads, 0, k_ref.shape[0])

    _turn_all(q_ref, qr_s, cos_ref, sin_ref, heads, iq * bq, bq)
    top_s[...] = jnp.full(top_s.shape, NEG, jnp.float32)
    mix_s[...] = jnp.zeros(mix_s.shape, jnp.float32)
    ones = jnp.ones((8, BLOCK), jnp.bfloat16)

    def block(j, some, diagonal):
        here = pl.ds(pl.multiple_of(j * BLOCK, BLOCK), BLOCK)
        now = [(i, n) for i, n in pieces if n in some]
        scores = [_dot(kr_s[here, _head(i)], qr_s[n * BLOCK : (n + 1) * BLOCK, _head(i)], 1, 1) for i, n in now]
        weights, keeps = [], []
        for (i, n), s in zip(now, scores):
            at = slice(n * BLOCK, (n + 1) * BLOCK)
            if n == diagonal:
                s = jnp.where(gap_s[...] >= 0, s, HIDDEN)
            old = top_s[i : i + 1, at]
            top = jnp.maximum(old, s.max(axis=0, keepdims=True))
            top_s[i : i + 1, at] = top
            weights.append(jnp.exp2((s - top) * e).astype(jnp.bfloat16))
            keeps.append(jnp.exp2((old - top) * e))
        for (i, n), p, keep in zip(now, weights, keeps):
            at = slice(n * BLOCK, (n + 1) * BLOCK)
            values = jnp.concatenate([v_ref[here, _head(i)].T, ones], axis=0)
            mix_s[i, :, at] = mix_s[i, :, at] * keep + _dot(values, p, 1, 0)

    lax.fori_loop(0, iq * strips, lambda j, _: block(j, range(strips), None), None)
    for n in range(strips):
        block(iq * strips + n, range(n, strips), n)
    for i in range(heads):
        top, total = top_s[i : i + 1, :], mix_s[i, HEAD : HEAD + 1, :]
        o_ref[:, _head(i)] = (mix_s[i, :HEAD, :] * (1 / total)).T.astype(o_ref.dtype)
        lse_ref[i : i + 1, :] = top * SCALE + jnp.log(total)


def _backward(q_ref, k_ref, v_ref, o_ref, do_ref, lse_ref, cos_ref, sin_ref, dq_ref, dk_ref, dv_ref, qr_s, kr_s, dq_s, dk_s, dv_s, gap_s, *, heads):
    iq = pl.program_id(0)
    e = SCALE * LOG2E

    @pl.when(iq == 0)
    def _():
        gap_s[...] = _gap()
        dk_s[...] = jnp.zeros_like(dk_s)
        dv_s[...] = jnp.zeros_like(dv_s)
        _turn_all(k_ref, kr_s, cos_ref, sin_ref, heads, 0, k_ref.shape[0])

    _turn_all(q_ref, qr_s, cos_ref, sin_ref, heads, iq * BLOCK, BLOCK)
    dq_s[...] = jnp.zeros_like(dq_s)
    lses = [lse_ref[i : i + 1, :] * LOG2E for i in range(heads)]
    deltas = [(do_ref[:, _head(i)].astype(jnp.float32) * o_ref[:, _head(i)].astype(jnp.float32)).T.sum(axis=0, keepdims=True) for i in range(heads)]

    def block(j, masked):
        here = pl.ds(pl.multiple_of(j * BLOCK, BLOCK), BLOCK)
        scores = [_dot(kr_s[here, _head(i)], qr_s[:, _head(i)], 1, 1) for i in range(heads)]
        dps = [_dot(v_ref[here, _head(i)], do_ref[:, _head(i)], 1, 1) for i in range(heads)]
        for i in range(heads):
            p = jnp.exp2(scores[i] * e - lses[i])
            if masked:
                p = jnp.where(gap_s[...] >= 0, p, 0.0)
            ds = (p * (dps[i] - deltas[i])).astype(jnp.bfloat16)
            dv_s[here, _head(i)] += _dot(p.astype(jnp.bfloat16), do_ref[:, _head(i)], 1, 0)
            dk_s[here, _head(i)] += _dot(ds, qr_s[:, _head(i)], 1, 0)
            dq_s[i] += _dot(kr_s[here, _head(i)].T, ds, 1, 0)

    lax.fori_loop(0, iq, lambda j, _: block(j, False), None)
    block(iq, True)
    place = pl.ds(pl.multiple_of(iq * BLOCK, BLOCK), BLOCK)
    for i in range(heads):
        dq_ref[:, _head(i)] = _turn((dq_s[i] * SCALE).T.astype(jnp.bfloat16), cos_ref[place, :], sin_ref[place, :], True)

    @pl.when(iq == pl.num_programs(0) - 1)
    def _():
        def strip(s, _):
            here = pl.ds(pl.multiple_of(s * 256, 256), 256)
            for i in range(heads):
                dk_ref[here, _head(i)] = _turn((dk_s[here, _head(i)] * SCALE).astype(jnp.bfloat16), cos_ref[here, :], sin_ref[here, :], True)
            dv_ref[here, :] = dv_s[here, :].astype(jnp.bfloat16)
        lax.fori_loop(0, dk_ref.shape[0] // 256, strip, None)


def _cost(tokens, heads, dots, arrays):
    return pl.CostEstimate(flops=tokens * tokens * heads * HEAD * dots, transcendentals=tokens * tokens * heads // 2, bytes_accessed=2 * tokens * heads * HEAD * arrays)


def attend(q, k, v, cos, sin):
    tokens, wide = q.shape
    heads, bq = wide // HEAD, min(FWD_STRIPS * BLOCK, tokens)
    rows = pl.BlockSpec((bq, wide), lambda i: (i, 0))
    every = pl.BlockSpec((tokens, wide), lambda i: (0, 0))
    table = pl.BlockSpec((tokens, HALF), lambda i: (0, 0))
    return pl.pallas_call(
        functools.partial(_forward, heads=heads),
        grid=(tokens // bq,),
        in_specs=[rows, every, every, table, table],
        out_specs=[rows, pl.BlockSpec((heads, bq), lambda i: (0, i))],
        out_shape=[jax.ShapeDtypeStruct((tokens, wide), q.dtype), jax.ShapeDtypeStruct((heads, tokens), jnp.float32)],
        scratch_shapes=[pltpu.VMEM((bq, wide), q.dtype), pltpu.VMEM((tokens, wide), q.dtype), pltpu.VMEM((heads, bq), jnp.float32),
                        pltpu.VMEM((heads, HEAD + 8, bq), jnp.float32), pltpu.VMEM((BLOCK, BLOCK), jnp.int32)],
        compiler_params=pltpu.CompilerParams(dimension_semantics=("arbitrary",), vmem_limit_bytes=VMEM),
        cost_estimate=_cost(tokens, heads, 2, 4),
    )(q, k, v, cos, sin)


def attend_bwd(q, k, v, out, d_out, lse, cos, sin):
    tokens, wide = q.shape
    heads = wide // HEAD
    rows = pl.BlockSpec((BLOCK, wide), lambda i: (i, 0))
    every = pl.BlockSpec((tokens, wide), lambda i: (0, 0))
    table = pl.BlockSpec((tokens, HALF), lambda i: (0, 0))
    return pl.pallas_call(
        functools.partial(_backward, heads=heads),
        grid=(tokens // BLOCK,),
        in_specs=[rows, every, every, rows, rows, pl.BlockSpec((heads, BLOCK), lambda i: (0, i)), table, table],
        out_specs=[rows, every, every],
        out_shape=[jax.ShapeDtypeStruct((tokens, wide), q.dtype)] * 3,
        scratch_shapes=[pltpu.VMEM((BLOCK, wide), q.dtype), pltpu.VMEM((tokens, wide), q.dtype), pltpu.VMEM((heads, HEAD, BLOCK), jnp.float32),
                        pltpu.VMEM((tokens, wide), jnp.float32), pltpu.VMEM((tokens, wide), jnp.float32), pltpu.VMEM((BLOCK, BLOCK), jnp.int32)],
        compiler_params=pltpu.CompilerParams(dimension_semantics=("arbitrary",), vmem_limit_bytes=VMEM),
        cost_estimate=_cost(tokens, heads, 5, 8),
    )(q, k, v, out, d_out, lse, cos, sin)


@jax.custom_vjp
def attention(q, k, v, cos, sin):
    return attend(q, k, v, cos, sin)[0]


def _attention_fwd(q, k, v, cos, sin):
    out, lse = attend(q, k, v, cos, sin)
    return out, (q, k, v, out, lse, cos, sin)


def _attention_bwd(kept, d_out):
    q, k, v, out, lse, cos, sin = kept
    return (*attend_bwd(q, k, v, out, d_out, lse, cos, sin), jnp.zeros_like(cos), jnp.zeros_like(sin))


attention.defvjp(_attention_fwd, _attention_bwd)


def matmul(a, w):
    return jnp.dot(a, w, preferred_element_type=jnp.float32).astype(jnp.bfloat16)


def normed(h):
    wide = h.astype(jnp.float32)
    scale = lax.rsqrt(jnp.mean(wide**2, -1, keepdims=True) + 1e-6)
    return (wide * scale).astype(jnp.bfloat16)


def angles(tokens):
    angle = jnp.arange(tokens, dtype=jnp.float32)[:, None] * THETA ** (-jnp.arange(HALF, dtype=jnp.float32) / HALF)
    return jnp.cos(angle), jnp.sin(angle)


def layer(h, w, cos, sin):
    a = normed(h)
    h = h + matmul(attention(*(matmul(a, w[name]) for name in ("wq", "wk", "wv")), cos, sin), w["wo"])
    b = normed(h)
    gate = jnp.dot(b, w["w_gate"], preferred_element_type=jnp.float32)
    up = jnp.dot(b, w["w_up"], preferred_element_type=jnp.float32)
    return h + matmul((jax.nn.silu(gate) * up).astype(jnp.bfloat16), w["w_down"])


def adamw(w, m, v, g):
    m = 0.9 * m + 0.1 * g
    v = 0.95 * v + 0.05 * g * g
    step = m * lax.rsqrt(v + 1e-8) + 0.1 * w
    return (w - 0.02 * step).astype(jnp.bfloat16), m, v


def clipped(gradients, sum_of_squares, count):
    factor = jnp.minimum(1.0, 0.5 * lax.rsqrt(sum_of_squares / count + 1e-30))
    return [g * factor for g in gradients]


SIZES = (2, 2, 4, 2)
STRIDES = (16, 8, 2, 1)
ORDERS = ((96, (0, 1, 2)), (96, (1, 2, 0)), (64, (2, 0, 1)))


def place():
    me = lax.axis_index("dp")
    return [lax.rem(lax.div(me, stride), size) for stride, size in zip(STRIDES, SIZES)]


def sent(t, axis, by):
    stride, size = STRIDES[axis], SIZES[axis]
    pairs = []
    for source in range(32):
        at = source // stride % size
        pairs.append((source, source + ((at + by) % size - at) * stride))
    return lax.ppermute(t, "dp", pairs)


def scattered(t, axis, dim, at):
    size = SIZES[axis]
    got = []
    for by in range(1, size):
        other = lax.dynamic_index_in_dim(t, lax.rem(at + by, size), dim, keepdims=False)
        got.append(sent(other.astype(jnp.bfloat16), axis, by))
    total = lax.dynamic_index_in_dim(t, at, dim, keepdims=False).astype(jnp.float32)
    for one in got:
        total = total + one.astype(jnp.float32)
    return total


def summed(pack):
    at = place()
    pack = scattered(pack, 3, 0, at[3])
    out, first = [], 0
    for rows, order in ORDERS:
        t = pack[..., first : first + rows, :]
        left = [0, 1, 2]
        for axis in order:
            t = scattered(t, axis, left.index(axis), at[axis])
            left.remove(axis)
        out.append(t)
        first += rows
    return jnp.concatenate(out, axis=0)


def everyone(t):
    for axis in (3, 0, 1, 2):
        got = [sent(t, axis, by) for by in range(1, SIZES[axis])]
        for one in got:
            t = t + one
    return t


def packed(g, n):
    rows, columns = g.shape
    g = g.reshape(n, rows // n, columns)
    return jnp.concatenate([g[:, :, at : at + 512] for at in range(0, columns, 512)], axis=1)


def unpacked(p, columns):
    pieces = columns // 512
    step = p.shape[-2] // pieces
    return jnp.concatenate([p[..., i * step : (i + 1) * step, :] for i in range(pieces)], axis=-1)


def solution(mesh):
    n = mesh.shape["dp"]

    def step(x, dy, *arrays):
        weights, m, v = (arrays[i : i + 7] for i in (0, 7, 14))
        layers = weights[0].shape[0]
        cos, sin = angles(x.shape[1])
        h, backs = x[0], []
        for number in range(layers):
            h, back = jax.vjp(lambda w, h: layer(h, w, cos, sin), {name: w[number] for name, w in zip(NAMES, weights, strict=True)}, h)
            backs.append(back)
        by_h, mine = dy[0], [None] * layers
        for number in reversed(range(layers)):
            by_w, by_h = backs[number](by_h)
            pack = jnp.concatenate([packed(by_w[name], n) for name in NAMES], axis=1)
            if number:
                by_h, pack = lax.optimization_barrier((by_h, pack))
                mine[number] = lax.psum_scatter(pack, "dp", scatter_dimension=0, tiled=False)
            else:
                pack = pack.reshape(16, 2, *pack.shape[1:]).transpose(1, 0, 2, 3).reshape(2, 2, 2, 4, *pack.shape[1:])
                mine[number] = summed(pack).astype(jnp.bfloat16)
        sums = [g.astype(jnp.float32) for g in mine]
        squares = everyone(sum(jnp.sum(g * g) for g in sums).reshape(1, 1))
        (factor,) = clipped([jnp.ones((), jnp.float32)], squares.reshape(()), n * sum(g.size for g in sums))
        me = lax.axis_index("dp")
        at, new = 0, []
        for name, w, m_, v_ in zip(NAMES, weights, m, v, strict=True):
            rows, columns = m_.shape[1:]
            own = lax.dynamic_slice_in_dim(w, me * rows, rows, 1).astype(jnp.float32)
            size = rows * columns // 512
            g = unpacked(jnp.stack([s[at : at + size] for s in sums]), columns)
            new.append(adamw(own, m_, v_, g * factor))
            at += size
        whole = lax.all_gather(jnp.concatenate([packed(one[0].reshape(-1, one[0].shape[-1]), layers) for one in new], axis=1), "dp", axis=0, tiled=False)
        out, at = [], 0
        for name, w, m_ in zip(NAMES, weights, m, strict=True):
            rows, columns = m_.shape[1:]
            size = rows * columns // 512
            got = unpacked(whole[:, :, at : at + size], columns)
            out.append(got.transpose(1, 0, 2, 3).reshape(w.shape))
            at += size
        return (*out, *(one[1] for one in new), *(one[2] for one in new))

    states, all_of, cut = P(("rep", "dp"), None, None), P(None, None, None), P(None, "dp", None)
    return jax.shard_map(
        step,
        mesh=mesh,
        in_specs=(states, states) + (all_of,) * 7 + (cut,) * 14,
        out_specs=(P("rep", None, None),) * 7 + (P("rep", "dp", None),) * 14,
        check_vma=False,
    )
```
